8 devices in a mesh: dp: 2 (over z, y), tp: 4 (over x, core).
Axes of the slice: x: 2, y: 2, z: 1, core: 2. Of those that a mesh axis runs over, the one named last changes fastest.
Arguments:
- hidden_in: bfloat16 [2048, 640], P(('dp', 'tp')), parts along dimension 0
- k_cache: bfloat16 [2048, 512, 256], P(('dp', 'tp')), parts along dimension 0
- v_cache: bfloat16 [2048, 512, 256], P(('dp', 'tp')), parts along dimension 0
- cache_len: int32 [2048], P(('dp', 'tp')), parts along dimension 0
- norm_attn: bfloat16 [640], replicated
- norm_mlp: bfloat16 [640], replicated
- w_q: bfloat16 [640, 1024], replicated
- w_k: bfloat16 [640, 256], replicated
- w_v: bfloat16 [640, 256], replicated
- w_o: bfloat16 [1024, 640], replicated
- w_gate: bfloat16 [640, 2048], P(None, 'tp')
- w_up: bfloat16 [640, 2048], P(None, 'tp')
- w_down: bfloat16 [2048, 640], P('tp')
Outputs:
- output 1: bfloat16 [2048, 640], P(('dp', 'tp')), parts along dimension 0
- output 2: bfloat16 [2048, 256], P(('dp', 'tp')), parts along dimension 0
- output 3: bfloat16 [2048, 256], P(('dp', 'tp')), parts along dimension 0
There are 2 independent parts. The reference program is written for one: setup_inputs(seed, part) draws one part's arguments, and reference() takes and returns one part's arrays. A program takes and returns all parts, laid end to end along the dimension named above; an argument that names none is the same for every part.
All inputs are finite; a program needn't handle non-finite values.
Results may differ from the reference program's by a relative error of at most 0.00492933.
Values are sent between devices in bfloat16 or wider.
A program may use at most 1 GiB of HBM per device.

```python
import jax
import jax.numpy as jnp
from jax import lax

D_MODEL = 640
NUM_HEADS = 4
HEAD_DIM = 256
FF_DIM = 2048
BATCH_ROWS = 1024
CACHE_SIZE = 512


def scaled_normal(key_w, shape_w, fan_in):
    return (jax.random.normal(key_w, shape_w, jnp.float32) * fan_in ** -0.5).astype(jnp.bfloat16)


def setup_inputs(seed: int = 0, part: int = 0) -> dict:
    base_key = jax.random.key(seed)
    shared_keys = jax.random.split(base_key, 9)
    own_keys = jax.random.split(jax.random.fold_in(base_key, part), 5)
    q_width = NUM_HEADS * HEAD_DIM
    hidden_in = jax.random.normal(own_keys[0], (BATCH_ROWS, D_MODEL), jnp.float32)
    k_cache = 2.0 * jax.random.normal(own_keys[1], (BATCH_ROWS, CACHE_SIZE, HEAD_DIM), jnp.float32)
    v_mean = 0.7 * jax.random.normal(own_keys[2], (BATCH_ROWS, 1, HEAD_DIM), jnp.float32)
    v_cache = v_mean + jax.random.normal(own_keys[3], (BATCH_ROWS, CACHE_SIZE, HEAD_DIM), jnp.float32)
    cache_len = jax.random.randint(own_keys[4], (BATCH_ROWS,), 0, CACHE_SIZE, jnp.int32)
    cache_len = cache_len.at[0].set(CACHE_SIZE - 1)
    return {
        'hidden_in': hidden_in.astype(jnp.bfloat16),
        'k_cache': k_cache.astype(jnp.bfloat16),
        'v_cache': v_cache.astype(jnp.bfloat16),
        'cache_len': cache_len,
        'norm_attn': (0.3 * jax.random.normal(shared_keys[0], (D_MODEL,), jnp.float32)).astype(jnp.bfloat16),
        'norm_mlp': (0.3 * jax.random.normal(shared_keys[1], (D_MODEL,), jnp.float32)).astype(jnp.bfloat16),
        'w_q': scaled_normal(shared_keys[2], (D_MODEL, q_width), D_MODEL),
        'w_k': scaled_normal(shared_keys[3], (D_MODEL, HEAD_DIM), D_MODEL),
        'w_v': scaled_normal(shared_keys[4], (D_MODEL, HEAD_DIM), D_MODEL),
        'w_o': scaled_normal(shared_keys[5], (q_width, D_MODEL), q_width),
        'w_gate': scaled_normal(shared_keys[6], (D_MODEL, FF_DIM), D_MODEL),
        'w_up': scaled_normal(shared_keys[7], (D_MODEL, FF_DIM), D_MODEL),
        'w_down': scaled_normal(shared_keys[8], (FF_DIM, D_MODEL), FF_DIM),
    }


def rms_scale(values, gain_vec):
    wide_vals = values.astype(jnp.float32)
    inv_rms = lax.rsqrt(jnp.mean(wide_vals * wide_vals, axis=-1, keepdims=True) + 1e-6)
    return (wide_vals * inv_rms * (1.0 + gain_vec.astype(jnp.float32))).astype(jnp.bfloat16)


def rope_tables(positions, head_dim):
    half_dim = head_dim // 2
    inv_freq = 10000.0 ** (-2.0 * jnp.arange(half_dim, dtype=jnp.float32) / head_dim)
    angles = positions.astype(jnp.float32)[:, None] * inv_freq[None, :]
    return jnp.cos(angles), jnp.sin(angles)


def rotary(values, cos_t, sin_t):
    half_dim = values.shape[-1] // 2
    first_half = values[..., :half_dim]
    second_half = values[..., half_dim:]
    return jnp.concatenate([first_half * cos_t - second_half * sin_t, second_half * cos_t + first_half * sin_t], axis=-1)


def attend_row(row_args):
    q_row, k_row, v_row, k_hist, v_hist, position = row_args
    q_wide = q_row.astype(jnp.float32)
    hist_score = jnp.einsum('hd,td->ht', q_wide, k_hist.astype(jnp.float32))
    new_score = jnp.einsum('hd,d->h', q_wide, k_row.astype(jnp.float32))
    valid_mask = jnp.arange(k_hist.shape[0]) < position
    hist_score = jnp.where(valid_mask[None, :], hist_score, -jnp.inf)
    peak_score = jnp.maximum(jnp.max(hist_score, axis=-1), new_score)
    hist_weight = jnp.exp(hist_score - peak_score[:, None])
    new_weight = jnp.exp(new_score - peak_score)
    weight_sum = jnp.sum(hist_weight, axis=-1) + new_weight
    hist_prob = (hist_weight / weight_sum[:, None]).astype(jnp.bfloat16)
    new_prob = (new_weight / weight_sum).astype(jnp.bfloat16)
    attn_out = jnp.einsum('ht,td->hd', hist_prob.astype(jnp.float32), v_hist.astype(jnp.float32))
    attn_out = attn_out + new_prob.astype(jnp.float32)[:, None] * v_row.astype(jnp.float32)[None, :]
    return attn_out.astype(jnp.bfloat16)


def reference(hidden_in, k_cache, v_cache, cache_len, norm_attn, norm_mlp, w_q, w_k, w_v, w_o, w_gate, w_up, w_down):
    num_rows = hidden_in.shape[0]
    normed = rms_scale(hidden_in, norm_attn)
    q_lin = jnp.dot(normed, w_q, preferred_element_type=jnp.float32).reshape(num_rows, NUM_HEADS, HEAD_DIM)
    k_lin = jnp.dot(normed, w_k, preferred_element_type=jnp.float32)
    v_new = jnp.dot(normed, w_v, preferred_element_type=jnp.float32).astype(jnp.bfloat16)
    cos_t, sin_t = rope_tables(cache_len, HEAD_DIM)
    q_rot = (rotary(q_lin, cos_t[:, None, :], sin_t[:, None, :]) * HEAD_DIM ** -0.5).astype(jnp.bfloat16)
    k_new = rotary(k_lin, cos_t, sin_t).astype(jnp.bfloat16)
    attn_out = lax.map(attend_row, (q_rot, k_new, v_new, k_cache, v_cache, cache_len))
    mixed = jnp.dot(attn_out.reshape(num_rows, NUM_HEADS * HEAD_DIM), w_o, preferred_element_type=jnp.float32)
    x_mid = hidden_in.astype(jnp.float32) + mixed
    xn_mid = rms_scale(x_mid, norm_mlp)
    gate_act = jnp.dot(xn_mid, w_gate, preferred_element_type=jnp.float32)
    up_act = jnp.dot(xn_mid, w_up, preferred_element_type=jnp.float32)
    hidden_act = (jax.nn.gelu(gate_act, approximate=True) * up_act).astype(jnp.bfloat16)
    down_sum = jnp.dot(hidden_act, w_down, preferred_element_type=jnp.float32)
    hidden_out = (x_mid + down_sum).astype(jnp.bfloat16)
    return hidden_out, k_new, v_new
```

```python
import functools

import jax
import jax.numpy as jnp
from jax import lax
from jax.experimental import pallas as pl
from jax.experimental.pallas import tpu as pltpu
from jax.sharding import PartitionSpec as P

HEADS = 4
HEAD_DIM = 256
HALF = HEAD_DIM // 2
GROUP = 8
RING = 8
BLOCK = 128
F32 = jnp.float32
BF16 = jnp.bfloat16


def rms_scale(values, gain_vec):
    wide_vals = values.astype(F32)
    inv_rms = lax.rsqrt(jnp.mean(wide_vals * wide_vals, axis=-1, keepdims=True) + 1e-6)
    return (wide_vals * inv_rms * (1.0 + gain_vec.astype(F32))).astype(BF16)


def dot(a, b):
    return jnp.dot(a, b, preferred_element_type=F32)


def dot_t(a, b):
    return lax.dot_general(a, b, (((1,), (1,)), ((), ())), preferred_element_type=F32)


def attn_kernel(rows, cache_size, x_ref, len_ref, na_ref, nm_ref, wq_ref, wk_ref, wv_ref, wo_ref, freq_ref, k_hbm, v_hbm,
                x1_ref, xn2_ref, knew_ref, vnew_ref,
                kbuf, vbuf, qg, ks, vs, lensb, s_buf, o_s, table, table_s, ksem, vsem, tsem):
    groups = rows // GROUP
    max_nb = cache_size // BLOCK

    len_row = len_ref[...].astype(F32)
    lane_id = lax.broadcasted_iota(jnp.int32, (1, rows), 1).astype(F32)
    key_row = len_row * rows + (rows - 1 - lane_id)
    key_col = jnp.broadcast_to(key_row, (128, rows)).T[:, :1]
    len_col = jnp.broadcast_to(len_row, (128, rows)).T[:, :1]
    sub_id = lax.broadcasted_iota(jnp.int32, (rows, rows), 0).astype(F32)
    lane_sq = lax.broadcasted_iota(jnp.int32, (rows, rows), 1).astype(F32)
    rank_row = jnp.sum((key_col > key_row).astype(F32), axis=0, keepdims=True)
    rank_col = jnp.sum((key_row > key_col).astype(F32), axis=1, keepdims=True)
    to_sorted = rank_row == sub_id
    to_natural = rank_col == lane_sq
    perm_row = jnp.sum(jnp.where(to_natural, sub_id, 0.0), axis=0, keepdims=True)
    slen_row = jnp.sum(jnp.where(to_natural, len_col, 0.0), axis=0, keepdims=True)
    slen_col = jnp.sum(jnp.where(to_sorted, len_row, 0.0), axis=1, keepdims=True)
    table[0:1, :] = (perm_row + rows * slen_row).astype(jnp.int32)
    table_copy = pltpu.make_async_copy(table.at[0:1], table_s, tsem)
    table_copy.start()
    lensb[...] = jnp.broadcast_to(slen_col, (rows, 128))

    zero = jnp.zeros((cache_size, HEAD_DIM), BF16)

    def clear(i, c):
        kbuf[i] = zero
        vbuf[i] = zero
        return c
    lax.fori_loop(0, RING * GROUP, clear, 0)
    table_copy.wait()

    def entry(pos):
        packed = table_s[0, pos]
        row = lax.rem(packed, rows)
        length = lax.div(packed, rows)
        size = jnp.maximum(lax.div(length + 15, 16) * 16, 16)
        return row, length, pl.multiple_of(size, 16)

    def k_copy(pos):
        row, _, size = entry(pos)
        slot = lax.rem(pos, RING * GROUP)
        return pltpu.make_async_copy(k_hbm.at[row, pl.ds(0, size)], kbuf.at[slot, pl.ds(0, size)], ksem.at[slot])

    def v_copy(pos):
        row, _, size = entry(pos)
        slot = lax.rem(pos, RING * GROUP)
        return pltpu.make_async_copy(v_hbm.at[row, pl.ds(0, size)], vbuf.at[slot, pl.ds(0, size)], vsem.at[slot])

    def issue(g):
        for b in range(GROUP):
            k_copy(g * GROUP + b).start()
            v_copy(g * GROUP + b).start()

    def wait_k(g):
        for b in range(GROUP):
            k_copy(g * GROUP + b).wait()

    def wait_v(g):
        for b in range(GROUP):
            v_copy(g * GROUP + b).wait()

    def prologue(g, c):
        issue(g)
        return c
    lax.fori_loop(0, RING, prologue, 0)

    xn = rms_scale(x_ref[...], na_ref[...])
    angles = len_col * freq_ref[...]
    cos_t, sin_t = jnp.cos(angles), jnp.sin(angles)

    def rotary(val):
        first, second = val[:, :HALF], val[:, HALF:]
        return jnp.concatenate([first * cos_t - second * sin_t, second * cos_t + first * sin_t], axis=-1)

    pick = to_sorted.astype(BF16)
    k_bf = rotary(dot(xn, wk_ref[...])).astype(BF16)
    v_bf = dot(xn, wv_ref[...]).astype(BF16)
    knew_ref[...] = k_bf
    vnew_ref[...] = v_bf
    ks[...] = dot(pick, k_bf)
    vs[...] = dot(pick, v_bf)
    for h in range(HEADS):
        q_h = (rotary(dot(xn, wq_ref[:, h * HEAD_DIM:(h + 1) * HEAD_DIM])) * HEAD_DIM ** -0.5).astype(BF16)
        q_s = dot(pick, q_h)
        qg[0:groups, h * GROUP:(h + 1) * GROUP, :] = q_s.reshape(groups, GROUP, HEAD_DIM)
    qg[groups] = jnp.zeros((HEADS * GROUP, HEAD_DIM), F32)

    def scores(g, nb):
        base = lax.rem(g, RING) * GROUP
        q = qg[g].astype(BF16)
        member = lax.broadcasted_iota(jnp.int32, (HEADS * GROUP, HEAD_DIM), 0) % GROUP
        out = None
        for b in range(GROUP):
            part = dot_t(jnp.where(member == b, q, jnp.zeros_like(q)), kbuf[base + b, :nb * BLOCK, :])
            out = part if out is None else out + part
        return out

    def finish(g, nb):
        width = nb * BLOCK
        base = lax.rem(g, RING) * GROUP
        start = pl.multiple_of(g * GROUP, GROUP)
        tile4 = lambda t: jnp.concatenate([t] * HEADS, axis=0)
        s = s_buf[:, :width]
        lens = tile4(lensb[pl.ds(start, GROUP), :])[:, :1]
        valid = lax.broadcasted_iota(jnp.int32, (HEADS * GROUP, width), 1).astype(F32) < lens
        q = qg[g]
        s_new = jnp.sum(q * tile4(ks[pl.ds(start, GROUP), :]), axis=-1, keepdims=True)
        s = jnp.where(valid, s, -jnp.inf)
        peak = jnp.maximum(jnp.max(s, axis=-1, keepdims=True), s_new)
        w = jnp.exp(s - peak)
        w_new = jnp.exp(s_new - peak)
        inv = 1.0 / (jnp.sum(w, axis=-1, keepdims=True) + w_new)
        prob = (w * inv).astype(BF16)
        prob_new = (w_new * inv).astype(BF16).astype(F32)
        member = lax.broadcasted_iota(jnp.int32, (HEADS * GROUP, width), 0) % GROUP
        out = None
        for b in range(GROUP):
            part = dot(jnp.where(member == b, prob, jnp.zeros_like(prob)), vbuf[base + b, :width, :])
            out = part if out is None else out + part
        out = out + prob_new * tile4(vs[pl.ds(start, GROUP), :])
        for h in range(HEADS):
            o_s[pl.ds(start, GROUP), h * HEAD_DIM:(h + 1) * HEAD_DIM] = out[h * GROUP:(h + 1) * GROUP]

    def blocks(g):
        length = lax.div(table_s[0, g * GROUP], rows)
        return jnp.maximum(lax.div(length + BLOCK - 1, BLOCK), 1)

    wait_k(0)
    s_buf[...] = scores(0, max_nb)

    def step(g, c):
        @pl.when(jnp.logical_and(g >= 1, g + RING - 1 < groups))
        def _():
            issue(g + RING - 1)
        wait_v(g)

        @pl.when(g + 1 < groups)
        def _():
            wait_k(g + 1)
        nb_g = blocks(g)
        for nb in range(1, max_nb + 1):
            @pl.when(nb_g == nb)
            def _():
                nxt = scores(g + 1, nb)
                finish(g, nb)
                s_buf[:, :nb * BLOCK] = nxt
        return c
    lax.fori_loop(0, groups, step, 0)

    back = to_natural.astype(BF16)
    mixed = None
    for h in range(HEADS):
        o_h = dot(back, o_s[:, h * HEAD_DIM:(h + 1) * HEAD_DIM].astype(BF16)).astype(BF16)
        part = dot(o_h, wo_ref[h * HEAD_DIM:(h + 1) * HEAD_DIM, :])
        mixed = part if mixed is None else mixed + part
    x1 = x_ref[...].astype(F32) + mixed
    x1_ref[...] = x1
    xn2_ref[...] = rms_scale(x1, nm_ref[...])


def attention(hidden_in, k_cache, v_cache, cache_len, norm_attn, norm_mlp, w_q, w_k, w_v, w_o):
    rows, d_model = hidden_in.shape
    cache_size = k_cache.shape[1]
    groups = rows // GROUP
    freq = 10000.0 ** (-2.0 * jnp.arange(HALF, dtype=F32) / HEAD_DIM)
    vmem = pl.BlockSpec(memory_space=pltpu.VMEM)
    hbm = pl.BlockSpec(memory_space=pl.ANY)
    return pl.pallas_call(
        functools.partial(attn_kernel, rows, cache_size),
        out_shape=(jax.ShapeDtypeStruct((rows, d_model), F32), jax.ShapeDtypeStruct((rows, d_model), BF16),
                   jax.ShapeDtypeStruct((rows, HEAD_DIM), BF16), jax.ShapeDtypeStruct((rows, HEAD_DIM), BF16)),
        in_specs=[vmem] * 9 + [hbm] * 2,
        out_specs=(vmem,) * 4,
        scratch_shapes=[
            pltpu.VMEM((RING * GROUP, cache_size, HEAD_DIM), BF16),
            pltpu.VMEM((RING * GROUP, cache_size, HEAD_DIM), BF16),
            pltpu.VMEM((groups + 1, HEADS * GROUP, HEAD_DIM), F32),
            pltpu.VMEM((rows, HEAD_DIM), F32),
            pltpu.VMEM((rows, HEAD_DIM), F32),
            pltpu.VMEM((rows, 128), F32),
            pltpu.VMEM((HEADS * GROUP, cache_size), F32),
            pltpu.VMEM((rows, HEADS * HEAD_DIM), F32),
            pltpu.VMEM((8, rows), jnp.int32),
            pltpu.SMEM((1, rows), jnp.int32),
            pltpu.SemaphoreType.DMA((RING * GROUP,)),
            pltpu.SemaphoreType.DMA((RING * GROUP,)),
            pltpu.SemaphoreType.DMA,
        ],
        compiler_params=pltpu.CompilerParams(vmem_limit_bytes=52 * 1024 * 1024),
        cost_estimate=pl.CostEstimate(flops=10 ** 10, bytes_accessed=7 * 10 ** 7, transcendentals=10 ** 6),
        name='attention',
    )(hidden_in, cache_len.reshape(1, rows), norm_attn.reshape(1, d_model), norm_mlp.reshape(1, d_model),
      w_q, w_k, w_v, w_o, freq.reshape(1, HALF), k_cache, v_cache)


CORE = [(0, 1), (1, 0), (2, 3), (3, 2)]
ACROSS = [(0, 2), (1, 3), (2, 0), (3, 1)]


def solution(mesh):
    row_spec = P(('dp', 'tp'), None)
    cache_spec = P(('dp', 'tp'), None, None)
    full_vec = P(None)
    full_mat = P(None, None)

    def per_device(hidden_in, k_cache, v_cache, cache_len, norm_attn, norm_mlp, w_q, w_k, w_v, w_o, w_gate, w_up, w_down):
        own = (w_gate, w_up, w_down)
        far = tuple(lax.ppermute(w, 'tp', ACROSS) for w in own)
        near = tuple(lax.ppermute(w, 'tp', CORE) for w in own)
        x_mid, xn_mid, k_new, v_new = attention(hidden_in, k_cache, v_cache, cache_len, norm_attn, norm_mlp, w_q, w_k, w_v, w_o)
        diag = tuple(lax.ppermute(w, 'tp', CORE) for w in far)
        total = x_mid
        for gate, up, down in (own, near, far, diag):
            gate_act = dot(xn_mid, gate)
            up_act = dot(xn_mid, up)
            hidden_act = (jax.nn.gelu(gate_act, approximate=True) * up_act).astype(BF16)
            total = total + dot(hidden_act, down)
        return total.astype(BF16), k_new, v_new

    return jax.shard_map(
        per_device,
        mesh=mesh,
        in_specs=(row_spec, cache_spec, cache_spec, P(('dp', 'tp')), full_vec, full_vec,
                  full_mat, full_mat, full_mat, full_mat, P(None, 'tp'), P(None, 'tp'), P('tp', None)),
        out_specs=(row_spec, row_spec, row_spec),
        check_vma=False,
    )
```

```python
import functools
import math

import jax
import jax.numpy as jnp
from jax import lax
from jax.experimental import pallas as pl
from jax.experimental.pallas import tpu as pltpu
from jax.sharding import PartitionSpec as P

HEADS = 4
HEAD_DIM = 256
HALF = HEAD_DIM // 2
GROUP = 16
RING = 4
TABLE = 512


def VIA_XLU(b):
    return b % 2 == 0

BLOCK = 128
STACK = HEADS * GROUP
F32 = jnp.float32
BF16 = jnp.bfloat16


def dot(a, b):
    return jnp.dot(a, b, preferred_element_type=F32)


def dot_t(a, b):
    return lax.dot_general(a, b, (((1,), (1,)), ((), ())), preferred_element_type=F32)


def rms_scale(wide_vals, gain):
    inv_rms = lax.rsqrt(jnp.mean(wide_vals * wide_vals, axis=-1, keepdims=True) + 1e-6)
    return (wide_vals * inv_rms * (1.0 + gain)).astype(BF16)


def tile_heads(t):
    return jnp.concatenate([t] * HEADS, axis=0)


def attend_groups(parity, count, cache_size, table, k_hbm, v_hbm, kbuf, vbuf, ksem, vsem, s_buf, p_buf, pn_buf,
                  load_q, load_k, load_v, load_len, store, prepare):
    max_nb = cache_size // BLOCK

    def first_row(p):
        return (2 * p + parity) * GROUP

    def slot_row(p, b):
        return pl.multiple_of(((p & (RING - 1)) * GROUP + b) * cache_size, cache_size)

    def issue(hbm, buf, sems, p):
        for b in range(GROUP):
            src = pl.multiple_of(table[0, first_row(p) + b], cache_size)
            size = pl.multiple_of(table[1, first_row(p) + b], 16)
            pltpu.make_async_copy(hbm.at[pl.ds(src, size)], buf.at[pl.ds(slot_row(p, b), size)],
                                  sems.at[p & (RING - 1)]).start()

    def wait(hbm, buf, sems, p):
        n = pl.multiple_of(table[3, first_row(p)], 16)
        pltpu.make_async_copy(hbm.at[pl.ds(0, n)], buf.at[pl.ds(0, n)], sems.at[p & (RING - 1)]).wait()

    def blocks(p):
        return (table[1, first_row(p)] + (BLOCK - 1)) >> 7

    zeros = jnp.zeros((BLOCK, HEAD_DIM), BF16)

    def fill(p, c):
        upto = jnp.where(p < 1, max_nb, blocks(jnp.maximum(p - 1, 0)))
        for b in range(GROUP):
            base = slot_row(p, b)
            own = (table[1, first_row(p) + b] + (BLOCK - 1)) >> 7

            def clear(t, c):
                at = pl.multiple_of(base + t * BLOCK, BLOCK)
                kbuf[pl.ds(at, BLOCK), :] = zeros
                vbuf[pl.ds(at, BLOCK), :] = zeros
                return c
            lax.fori_loop(own - 1, upto, clear, 0)
        issue(k_hbm, kbuf, ksem, p)
        issue(v_hbm, vbuf, vsem, p)
        return c
    lax.fori_loop(0, RING, fill, 0)

    prepare()

    def scores(p, nb):
        q = load_q(2 * p + parity)
        member = lax.broadcasted_iota(jnp.int32, (STACK, HEAD_DIM), 0) % GROUP
        out = None
        for b in range(GROUP):
            k_b = kbuf[pl.ds(slot_row(p, b), nb * BLOCK), :]
            q_b = jnp.where(member == b, q, jnp.zeros_like(q))
            if VIA_XLU(b):
                k_t = k_b.T
                lane = lax.broadcasted_iota(jnp.int32, k_t.shape, 1)
                part = dot(q_b, jnp.where(lane < table[1, first_row(p) + b], k_t, jnp.zeros_like(k_t)))
            else:
                part = dot_t(q_b, k_b)
            out = part if out is None else out + part
        return out

    def softmax(p, s):
        width = s.shape[1]
        start = pl.multiple_of(first_row(p), GROUP)
        lens = tile_heads(load_len(start))[:, :1]
        valid = lax.broadcasted_iota(jnp.int32, (STACK, width), 1).astype(F32) < lens
        s_new = jnp.sum(load_q(2 * p + parity).astype(F32) * tile_heads(load_k(start)), axis=-1, keepdims=True)
        s = jnp.where(valid, s, -jnp.inf)
        peak = jnp.maximum(jnp.max(s, axis=-1, keepdims=True), s_new)
        w = jnp.exp(s - peak)
        w_new = jnp.exp(s_new - peak)
        inv = 1.0 / (jnp.sum(w, axis=-1, keepdims=True) + w_new)
        prob_new = (w_new * inv).astype(BF16).astype(F32)
        return (w * inv).astype(BF16), jnp.broadcast_to(prob_new, (STACK, 128))

    def values(p, prob, prob_new):
        width = prob.shape[1]
        start = pl.multiple_of(first_row(p), GROUP)
        member = lax.broadcasted_iota(jnp.int32, (STACK, width), 0) % GROUP
        out = None
        for b in range(GROUP):
            part = dot(jnp.where(member == b, prob, jnp.zeros_like(prob)), vbuf[pl.ds(slot_row(p, b), width), :])
            out = part if out is None else out + part
        store(p, out + prob_new[:, :1] * tile_heads(load_v(start)))

    wait(k_hbm, kbuf, ksem, 0)
    s_buf[...] = scores(0, max_nb)
    issue(k_hbm, kbuf, ksem, RING)

    def step(p, c):
        nb_p = blocks(p)
        wait(k_hbm, kbuf, ksem, p + 1)
        for nb in range(1, max_nb + 1):
            @pl.when(nb_p == nb)
            def _():
                width = nb * BLOCK
                nxt = scores(p + 1, nb)
                prob, prob_new = softmax(p, s_buf[:, :width])
                s_buf[:, :width] = nxt
                p_buf[:, :width] = prob
                pn_buf[...] = prob_new
        issue(k_hbm, kbuf, ksem, p + 1 + RING)
        wait(v_hbm, vbuf, vsem, p)
        for nb in range(1, max_nb + 1):
            @pl.when(nb_p == nb)
            def _():
                width = nb * BLOCK
                values(p, p_buf[:, :width], pn_buf[...])
        issue(v_hbm, vbuf, vsem, p + RING)
        return c
    lax.fori_loop(0, count, step, 0)


def first_kernel(rows, cache_size, x_in, len_in, na_ref, wq, wk, wv, k_hbm, v_hbm,
                 knew_ref, vnew_ref, table_out, q_out, ks_out, vs_out, len_out, o_out,
                 kbuf, vbuf, s_buf, p_buf, pn_buf, table, ksem, vsem, tsem):
    groups = rows // GROUP

    len_row = len_in[...].astype(F32)
    lane_id = lax.broadcasted_iota(jnp.int32, (1, rows), 1).astype(F32)
    key_row = len_row * rows + (rows - 1 - lane_id)
    key_col = jnp.broadcast_to(key_row, (128, rows)).T[:, :1]
    len_col = jnp.broadcast_to(len_row, (128, rows)).T[:, :1]
    sub_id = lax.broadcasted_iota(jnp.int32, (rows, rows), 0).astype(F32)
    lane_sq = lax.broadcasted_iota(jnp.int32, (rows, rows), 1).astype(F32)
    rank_row = jnp.sum((key_col > key_row).astype(F32), axis=0, keepdims=True)
    rank_col = jnp.sum((key_row > key_col).astype(F32), axis=1, keepdims=True)
    to_natural = rank_col == lane_sq
    perm_row = jnp.sum(jnp.where(to_natural, sub_id, 0.0), axis=0, keepdims=True).astype(jnp.int32)
    slen_row = jnp.sum(jnp.where(to_natural, len_col, 0.0), axis=0, keepdims=True).astype(jnp.int32)
    table_out[...] = jnp.zeros(table_out.shape, jnp.int32)
    size_row = jnp.maximum((slen_row + 15) & -16, 16)
    group_row = size_row
    for shift in (1, 2, 4, 8):
        group_row = group_row + pltpu.roll(group_row, rows - shift, 1)
    table_out[0:1, :rows] = perm_row * cache_size
    table_out[1:2, :rows] = size_row
    table_out[2:3, :rows] = perm_row
    table_out[3:4, :rows] = group_row
    table_copy = pltpu.make_async_copy(table_out, table, tsem)
    table_copy.start()
    table_copy.wait()

    def prepare():
        to_sorted = rank_row == sub_id
        slen_col = jnp.sum(jnp.where(to_sorted, len_row, 0.0), axis=1, keepdims=True)
        len_out[:rows, :] = jnp.broadcast_to(slen_col, (rows, 128))
        xn = rms_scale(x_in[...].astype(F32), na_ref[...].astype(F32))
        lane = lax.broadcasted_iota(jnp.int32, (1, HALF), 1).astype(F32)
        angles = len_col * jnp.exp(lane * (-2.0 / HEAD_DIM * math.log(10000.0)))
        cos_t, sin_t = jnp.cos(angles), jnp.sin(angles)

        def rotary(val):
            first, second = val[:, :HALF], val[:, HALF:]
            return jnp.concatenate([first * cos_t - second * sin_t, second * cos_t + first * sin_t], axis=-1)

        pick = to_sorted.astype(BF16)
        k_bf = rotary(dot(xn, wk[...])).astype(BF16)
        v_bf = dot(xn, wv[...]).astype(BF16)
        knew_ref[...] = k_bf
        vnew_ref[...] = v_bf
        ks_out[:rows, :] = dot(pick, k_bf)
        vs_out[:rows, :] = dot(pick, v_bf)
        for h in range(HEADS):
            q_h = (rotary(dot(xn, wq[:, h * HEAD_DIM:(h + 1) * HEAD_DIM])) * HEAD_DIM ** -0.5).astype(BF16)
            q_out[0:groups, h * GROUP:(h + 1) * GROUP, :] = dot(pick, q_h).reshape(groups, GROUP, HEAD_DIM)
        for g in range(groups, groups + 4):
            q_out[g] = jnp.zeros((STACK, HEAD_DIM), F32)
        pad = 2 * GROUP
        ks_out[rows:, :] = jnp.zeros((pad, HEAD_DIM), F32)
        vs_out[rows:, :] = jnp.zeros((pad, HEAD_DIM), F32)
        len_out[rows:, :] = jnp.zeros((pad, 128), F32)

    def store(p, out):
        for h in range(HEADS):
            o_out[pl.ds(pl.multiple_of(p * GROUP, GROUP), GROUP), h * HEAD_DIM:(h + 1) * HEAD_DIM] = out[h * GROUP:(h + 1) * GROUP]

    attend_groups(0, groups // 2, cache_size, table, k_hbm, v_hbm, kbuf, vbuf, ksem, vsem, s_buf, p_buf, pn_buf,
                  lambda g: q_out[g].astype(BF16), lambda s: ks_out[pl.ds(s, GROUP), :], lambda s: vs_out[pl.ds(s, GROUP), :],
                  lambda s: len_out[pl.ds(s, GROUP), :], store, prepare)


def second_kernel(rows, cache_size, table, x_in, q_in, ks_in, vs_in, len_in, o_even, nm_ref, tab_in, wo, k_hbm, v_hbm,
                  x1_ref, xn2_ref,
                  kbuf, vbuf, o_odd, s_buf, p_buf, pn_buf, ksem, vsem):
    groups = rows // GROUP

    def prepare():
        pass

    def store(p, out):
        for h in range(HEADS):
            o_odd[pl.ds(pl.multiple_of(p * GROUP, GROUP), GROUP), h * HEAD_DIM:(h + 1) * HEAD_DIM] = out[h * GROUP:(h + 1) * GROUP]

    attend_groups(1, groups // 2, cache_size, table, k_hbm, v_hbm, kbuf, vbuf, ksem, vsem, s_buf, p_buf, pn_buf,
                  lambda g: q_in[g].astype(BF16), lambda s: ks_in[pl.ds(s, GROUP), :], lambda s: vs_in[pl.ds(s, GROUP), :],
                  lambda s: len_in[pl.ds(s, GROUP), :], store, prepare)

    perm = tab_in[2:3, :rows]
    natural = lax.broadcasted_iota(jnp.int32, (rows, rows), 0)
    back = (natural == perm).astype(BF16)
    o_all = jnp.concatenate([o_even[...].reshape(groups // 2, GROUP, HEADS * HEAD_DIM),
                             o_odd[...].reshape(groups // 2, GROUP, HEADS * HEAD_DIM)], axis=1).reshape(rows, HEADS * HEAD_DIM).astype(BF16)
    mixed = dot(dot(back, o_all).astype(BF16), wo[...])
    x1 = x_in[...].astype(F32) + mixed
    x1_ref[...] = x1
    xn2_ref[...] = rms_scale(x1, nm_ref[...].astype(F32))


def shape(dims, dtype):
    return jax.ShapeDtypeStruct(dims, dtype)


VMEM_SPEC = pl.BlockSpec(memory_space=pltpu.VMEM)
SMEM_SPEC = pl.BlockSpec(memory_space=pltpu.SMEM)
HBM_SPEC = pl.BlockSpec(memory_space=pl.ANY)


def ring_scratch(cache_size):
    return [pltpu.VMEM((RING * GROUP * cache_size, HEAD_DIM), BF16)] * 2


def attention_first(hidden_in, k_cache, v_cache, cache_len, norm_attn, w_q, w_k, w_v):
    rows, d_model = hidden_in.shape
    cache_size = k_cache.shape[1]
    groups = rows // GROUP
    width = HEADS * HEAD_DIM
    k_flat = k_cache.reshape(rows * cache_size, HEAD_DIM)
    v_flat = v_cache.reshape(rows * cache_size, HEAD_DIM)
    params = pltpu.CompilerParams(vmem_limit_bytes=44 * 1024 * 1024)
    cost = pl.CostEstimate(flops=10 ** 10, bytes_accessed=4 * 10 ** 7, transcendentals=10 ** 6)
    sems = [pltpu.SemaphoreType.DMA((RING,)), pltpu.SemaphoreType.DMA((RING,))]
    return pl.pallas_call(
        functools.partial(first_kernel, rows, cache_size),
        out_shape=(shape((rows, HEAD_DIM), BF16), shape((rows, HEAD_DIM), BF16), shape((8, TABLE), jnp.int32),
                   shape((groups + 4, STACK, HEAD_DIM), F32), shape((rows + 2 * GROUP, HEAD_DIM), F32), shape((rows + 2 * GROUP, HEAD_DIM), F32),
                   shape((rows + 2 * GROUP, 128), F32), shape((rows // 2, width), F32)),
        in_specs=[VMEM_SPEC] * 6 + [HBM_SPEC] * 2,
        out_specs=(VMEM_SPEC,) * 8,
        scratch_shapes=ring_scratch(cache_size) + [
            pltpu.VMEM((STACK, cache_size), F32),
            pltpu.VMEM((STACK, cache_size), BF16),
            pltpu.VMEM((STACK, 128), F32),
            pltpu.SMEM((8, TABLE), jnp.int32),
        ] + sems + [pltpu.SemaphoreType.DMA],
        compiler_params=params,
        cost_estimate=cost,
        name='attention_first',
    )(hidden_in, cache_len.reshape(1, rows), norm_attn.reshape(1, d_model), w_q, w_k, w_v, k_flat, v_flat)


def attention_second(hidden_in, k_cache, v_cache, norm_mlp, w_o, table, q_s, k_s, v_s, len_s, o_even):
    rows, d_model = hidden_in.shape
    cache_size = k_cache.shape[1]
    groups = rows // GROUP
    width = HEADS * HEAD_DIM
    k_flat = k_cache.reshape(rows * cache_size, HEAD_DIM)
    v_flat = v_cache.reshape(rows * cache_size, HEAD_DIM)
    params = pltpu.CompilerParams(vmem_limit_bytes=44 * 1024 * 1024)
    cost = pl.CostEstimate(flops=10 ** 10, bytes_accessed=4 * 10 ** 7, transcendentals=10 ** 6)
    sems = [pltpu.SemaphoreType.DMA((RING,)), pltpu.SemaphoreType.DMA((RING,))]
    return pl.pallas_call(
        functools.partial(second_kernel, rows, cache_size),
        out_shape=(shape((rows, d_model), F32), shape((rows, d_model), BF16)),
        in_specs=[SMEM_SPEC] + [VMEM_SPEC] * 9 + [HBM_SPEC] * 2,
        out_specs=(VMEM_SPEC,) * 2,
        scratch_shapes=ring_scratch(cache_size) + [
            pltpu.VMEM((rows // 2, width), F32),
            pltpu.VMEM((STACK, cache_size), F32),
            pltpu.VMEM((STACK, cache_size), BF16),
            pltpu.VMEM((STACK, 128), F32),
        ] + sems,
        compiler_params=params,
        cost_estimate=cost,
        name='attention_second',
    )(table, hidden_in, q_s, k_s, v_s, len_s, o_even, norm_mlp.reshape(1, d_model), table, w_o, k_flat, v_flat)


def attention(hidden_in, k_cache, v_cache, cache_len, norm_attn, norm_mlp, w_q, w_k, w_v, w_o):
    k_new, v_new, *state = attention_first(hidden_in, k_cache, v_cache, cache_len, norm_attn, w_q, w_k, w_v)
    x1, xn2 = attention_second(hidden_in, k_cache, v_cache, norm_mlp, w_o, *state)
    return x1, xn2, k_new, v_new


def gelu(x):
    return 0.5 * x * (1.0 + jnp.tanh(math.sqrt(2.0 / math.pi) * (x + 0.044715 * (x * x * x))))


def mlp_kernel(shards, last, swap_at, *refs):
    x1_ref, xn_ref = refs[0], refs[1]
    weights = refs[2:2 + 3 * shards]
    out_ref = refs[2 + 3 * shards]
    straight = lax.axis_index('dp') == 0
    xn = xn_ref[...]
    total = x1_ref[...]
    for i in range(shards):
        first, second, down = weights[3 * i:3 * i + 3]
        parts = []
        for half in range(2):
            cols = slice(half * 256, half * 256 + 256)
            gate_act = dot(xn, first[:, cols])
            up_act = dot(xn, second[:, cols])
            if i == swap_at:
                gate_act, up_act = jnp.where(straight, gate_act, up_act), jnp.where(straight, up_act, gate_act)
            parts.append((gelu(gate_act) * up_act).astype(BF16))
        total = total + dot(jnp.concatenate(parts, axis=1), down[...])
    out_ref[...] = total.astype(out_ref.dtype)


def mlp(x1, xn, shards, last, swap_at):
    rows, d_model = xn.shape
    units = shards[0][0].shape[1]
    n = len(shards)
    return pl.pallas_call(
        functools.partial(mlp_kernel, n, last, swap_at),
        out_shape=shape((rows, d_model), BF16 if last else F32),
        in_specs=[VMEM_SPEC] * (2 + 3 * n),
        out_specs=VMEM_SPEC,
        compiler_params=pltpu.CompilerParams(vmem_limit_bytes=24 * 1024 * 1024),
        cost_estimate=pl.CostEstimate(flops=6 * rows * d_model * units * n, bytes_accessed=6 * d_model * units * n, transcendentals=rows * units * n),
        name='mlp',
    )(x1, xn, *[w for triple in shards for w in triple])


CORE = [(0, 1), (1, 0), (2, 3), (3, 2)]
ACROSS = [(0, 2), (1, 3), (2, 0), (3, 1)]
ROWS = [(0, 1), (1, 0)]


def solution(mesh):
    row_spec = P(('dp', 'tp'), None)
    cache_spec = P(('dp', 'tp'), None, None)
    full_vec = P(None)
    full_mat = P(None, None)

    def per_device(hidden_in, k_cache, v_cache, cache_len, norm_attn, norm_mlp, w_q, w_k, w_v, w_o, w_gate, w_up, w_down):
        half = jnp.where(lax.axis_index('dp') == 0, w_gate, w_up)
        half_far = lax.ppermute(half, 'tp', ACROSS)
        near = tuple(lax.ppermute(w, 'tp', CORE) for w in (w_gate, w_up, w_down))
        k_new, v_new, *state = attention_first(hidden_in, k_cache, v_cache, cache_len, norm_attn, w_q, w_k, w_v)
        half_far, down_own, state = lax.optimization_barrier((half_far, w_down, state))
        other_far = lax.ppermute(half_far, 'dp', ROWS)
        down_far = lax.ppermute(down_own, 'tp', ACROSS)
        half_diag = lax.ppermute(half_far, 'tp', CORE)
        x_mid, xn_mid = attention_second(hidden_in, k_cache, v_cache, norm_mlp, w_o, *state)
        other_far, down_far, x_mid, xn_mid = lax.optimization_barrier((other_far, down_far, x_mid, xn_mid))
        other_diag = lax.ppermute(other_far, 'tp', CORE)
        down_diag = lax.ppermute(down_far, 'tp', CORE)
        part = mlp(x_mid, xn_mid, ((w_gate, w_up, w_down), near, (half_far, other_far, down_far)), False, 2)
        out = mlp(part, xn_mid, ((half_diag, other_diag, down_diag),), True, 0)
        return out, k_new, v_new

    return jax.shard_map(
        per_device,
        mesh=mesh,
        in_specs=(row_spec, cache_spec, cache_spec, P(('dp', 'tp')), full_vec, full_vec,
                  full_mat, full_mat, full_mat, full_mat, P(None, 'tp'), P(None, 'tp'), P('tp', None)),
        out_specs=(row_spec, row_spec, row_spec),
        check_vma=False,
    )
```

```python
import functools
import math

import jax
import jax.numpy as jnp
from jax import lax
from jax.experimental import pallas as pl
from jax.experimental.pallas import tpu as pltpu
from jax.sharding import PartitionSpec as P

HEADS = 4
HEAD_DIM = 256
HALF = HEAD_DIM // 2
GROUP = 16
RING = 4
TABLE = 512
LEAD = 4 * GROUP


def turned(b):
    return b % 4 != 0


BLOCK = 128
STACK = HEADS * GROUP
F32 = jnp.float32
BF16 = jnp.bfloat16


def dot(a, b):
    return jnp.dot(a, b, preferred_element_type=F32)


def dot_t(a, b):
    return lax.dot_general(a, b, (((1,), (1,)), ((), ())), preferred_element_type=F32)


def rms_scale(wide_vals, gain):
    inv_rms = lax.rsqrt(jnp.mean(wide_vals * wide_vals, axis=-1, keepdims=True) + 1e-6)
    return (wide_vals * inv_rms * (1.0 + gain)).astype(BF16)


def tile_heads(t):
    return jnp.concatenate([t] * HEADS, axis=0)


def build_table(rows, cache_size, perm_row, slen_row, table):
    lane = lax.broadcasted_iota(jnp.int32, (1, TABLE), 1)

    def shifted(row):
        wide = jnp.concatenate([row, jnp.zeros((1, TABLE - rows), jnp.int32)], axis=1)
        return pltpu.roll(wide, LEAD, 1)

    def ahead(row, n):
        return pltpu.roll(row, TABLE - n, 1)

    real = jnp.logical_and(lane >= LEAD, lane < LEAD + rows)
    blocks = shifted(jnp.maximum((slen_row + (BLOCK - 1)) >> 7, 1))
    for step in (8, 4, 2, 1):
        blocks = jnp.where((lane & (GROUP - 1)) + step < GROUP, jnp.maximum(blocks, ahead(blocks, step)), blocks)
    k_blocks = ahead(blocks, LEAD)
    v_blocks = jnp.maximum(blocks, 1)
    v_blocks = jnp.where(k_blocks - v_blocks > 1, k_blocks, v_blocks)
    padded = (shifted(slen_row) + 15) & -16
    k_size = jnp.where(real, jnp.maximum(jnp.maximum(padded, 16), (blocks - 1) * BLOCK), 0)
    v_size = jnp.where(real, jnp.maximum(jnp.maximum(padded, 16), (v_blocks - 1) * BLOCK), 0)
    k_total, v_total = k_size, v_size
    for step in (1, 2, 4, 8):
        k_total = k_total + ahead(k_total, step)
        v_total = v_total + ahead(v_total, step)
    table[...] = jnp.zeros(table.shape, jnp.int32)
    table[0:1, :] = shifted(perm_row * cache_size)
    table[1:2, :] = k_size
    table[2:3, :] = v_size
    table[3:4, :] = v_blocks * 8 + k_blocks
    table[5:6, :] = k_total
    table[6:7, :] = v_total
    table[4:5, :rows] = perm_row


def attend_groups(parity, count, cache_size, table, k_hbm, v_hbm, kbuf, vbuf, ksem, vsem, s_buf, p_buf, pn_buf,
                  load_q, load_k, load_v, load_len, store, prepare):
    max_nb = cache_size // BLOCK

    def first_row(p):
        return (2 * p + parity) * GROUP

    def slot_row(p, b):
        return pl.multiple_of(((p & (RING - 1)) * GROUP + b) * cache_size, cache_size)

    def issue(which, p):
        hbm, buf, sems = ((k_hbm, kbuf, ksem), (v_hbm, vbuf, vsem))[which]
        for b in range(GROUP):
            src = pl.multiple_of(table[0, first_row(p) + (LEAD + b)], cache_size)
            size = pl.multiple_of(table[1 + which, first_row(p) + (LEAD + b)], 16)
            pltpu.make_async_copy(hbm.at[pl.ds(src, size)], buf.at[pl.ds(slot_row(p, b), size)],
                                  sems.at[p & (RING - 1)]).start()

    def wait(which, p):
        hbm, buf, sems = ((k_hbm, kbuf, ksem), (v_hbm, vbuf, vsem))[which]
        n = pl.multiple_of(table[5 + which, first_row(p) + LEAD], 16)
        pltpu.make_async_copy(hbm.at[pl.ds(0, n)], buf.at[pl.ds(0, n)], sems.at[p & (RING - 1)]).wait()

    token = lax.broadcasted_iota(jnp.int32, (BLOCK, HEAD_DIM), 0).astype(BF16)

    def read(which, p, b, nb):
        buf = (kbuf, vbuf)[which]
        at = slot_row(p, b)
        left = table[1 + which, first_row(p) + (LEAD + b)] - (nb - 1) * BLOCK
        tail = buf[pl.ds(at + (nb - 1) * BLOCK, BLOCK), :]
        tail = jnp.where(token < left.astype(F32).astype(BF16), tail, jnp.zeros_like(tail))
        if nb == 1:
            return tail
        return jnp.concatenate([buf[pl.ds(at, (nb - 1) * BLOCK), :], tail], axis=0)

    for p in range(3):
        issue(0, p)
    issue(1, 0)

    prepare()

    def score_part(p, b, nb, q, member):
        q_b = jnp.where(member == b, q, jnp.zeros_like(q))
        if turned(b):
            k_t = kbuf[pl.ds(slot_row(p, b), nb * BLOCK), :].T
            lane = lax.broadcasted_iota(jnp.int32, k_t.shape, 1)
            return dot(q_b, jnp.where(lane < table[1, first_row(p) + (LEAD + b)], k_t, jnp.zeros_like(k_t)))
        return dot_t(q_b, read(0, p, b, nb))

    def softmax(p):
        start = pl.multiple_of(first_row(p), GROUP)
        lens = tile_heads(load_len(start))[:, :1]
        valid = lax.broadcasted_iota(jnp.int32, s_buf.shape, 1).astype(F32) < lens
        s_new = jnp.sum(load_q(2 * p + parity).astype(F32) * tile_heads(load_k(start)), axis=-1, keepdims=True)
        s = jnp.where(valid, s_buf[...], -jnp.inf)
        peak = jnp.maximum(jnp.max(s, axis=-1, keepdims=True), s_new)
        w = jnp.exp(s - peak)
        w_new = jnp.exp(s_new - peak)
        inv = 1.0 / (jnp.sum(w, axis=-1, keepdims=True) + w_new)
        prob_new = (w_new * inv).astype(BF16).astype(F32)
        return (w * inv).astype(BF16), jnp.broadcast_to(prob_new, (STACK, 128))

    def work(p, v_nb, k_nb):
        prob, prob_new = softmax(jnp.maximum(p + 1, 0))
        q = load_q(2 * (p + 2) + parity)
        member_q = lax.broadcasted_iota(jnp.int32, (STACK, HEAD_DIM), 0) % GROUP
        old = p_buf[:, :v_nb * BLOCK]
        member = lax.broadcasted_iota(jnp.int32, old.shape, 0) % GROUP
        s, out = None, None
        for b in range(GROUP):
            if k_nb:
                part = score_part(p + 2, b, k_nb, q, member_q)
                s = part if s is None else s + part
            part = dot(jnp.where(member == b, old, jnp.zeros_like(old)), read(1, p, b, v_nb))
            out = part if out is None else out + part
        start = pl.multiple_of(first_row(jnp.maximum(p, 0)), GROUP)
        store(p + 2, out + pn_buf[:, :1] * tile_heads(load_v(start)))
        if k_nb:
            s_buf[:, :k_nb * BLOCK] = s
        p_buf[...] = prob
        pn_buf[...] = prob_new

    variants = [(v, k) for v in range(1, max_nb + 1) for k in (0, v, v + 1) if k <= max_nb]

    def step(i, c):
        p = i - 2
        wait(0, p + 2)
        wait(1, p)
        issue(1, p + 3)
        issue(0, p + 5)
        code = table[3, first_row(p) + LEAD]
        for v, k in variants:
            @pl.when(code == v * 8 + k)
            def _():
                work(p, v, k)
        return c
    lax.fori_loop(0, count + 2, step, 0)


def first_kernel(rows, cache_size, x_in, len_in, na_ref, wq, wk, wv, k_hbm, v_hbm,
                 knew_ref, vnew_ref, table_out, q_out, ks_out, vs_out, len_out, o_out,
                 kbuf, vbuf, s_buf, p_buf, pn_buf, table, ksem, vsem, tsem):
    groups = rows // GROUP

    len_row = len_in[...].astype(F32)
    lane_id = lax.broadcasted_iota(jnp.int32, (1, rows), 1).astype(F32)
    key_row = len_row * rows + lane_id
    key_col = jnp.broadcast_to(key_row, (128, rows)).T[:, :1]
    len_col = jnp.broadcast_to(len_row, (128, rows)).T[:, :1]
    sub_id = lax.broadcasted_iota(jnp.int32, (rows, rows), 0).astype(F32)
    lane_sq = lax.broadcasted_iota(jnp.int32, (rows, rows), 1).astype(F32)
    rank_row = jnp.sum((key_col < key_row).astype(F32), axis=0, keepdims=True)
    rank_col = jnp.sum((key_row < key_col).astype(F32), axis=1, keepdims=True)
    to_natural = rank_col == lane_sq
    perm_row = jnp.sum(jnp.where(to_natural, sub_id, 0.0), axis=0, keepdims=True).astype(jnp.int32)
    slen_row = jnp.sum(jnp.where(to_natural, len_col, 0.0), axis=0, keepdims=True).astype(jnp.int32)
    build_table(rows, cache_size, perm_row, slen_row, table_out)
    table_copy = pltpu.make_async_copy(table_out, table, tsem)
    table_copy.start()
    table_copy.wait()

    def prepare():
        to_sorted = rank_row == sub_id
        slen_col = jnp.sum(jnp.where(to_sorted, len_row, 0.0), axis=1, keepdims=True)
        len_out[:rows, :] = jnp.broadcast_to(slen_col, (rows, 128))
        xn = rms_scale(x_in[...].astype(F32), na_ref[...].astype(F32))
        lane = lax.broadcasted_iota(jnp.int32, (1, HALF), 1).astype(F32)
        angles = len_col * jnp.exp(lane * (-2.0 / HEAD_DIM * math.log(10000.0)))
        cos_t, sin_t = jnp.cos(angles), jnp.sin(angles)

        def rotary(val):
            first, second = val[:, :HALF], val[:, HALF:]
            return jnp.concatenate([first * cos_t - second * sin_t, second * cos_t + first * sin_t], axis=-1)

        pick = to_sorted.astype(BF16)
        k_bf = rotary(dot(xn, wk[...])).astype(BF16)
        v_bf = dot(xn, wv[...]).astype(BF16)
        knew_ref[...] = k_bf
        vnew_ref[...] = v_bf
        ks_out[:rows, :] = dot(pick, k_bf)
        vs_out[:rows, :] = dot(pick, v_bf)
        for h in range(HEADS):
            q_h = (rotary(dot(xn, wq[:, h * HEAD_DIM:(h + 1) * HEAD_DIM])) * HEAD_DIM ** -0.5).astype(BF16)
            q_out[0:groups, h * GROUP:(h + 1) * GROUP, :] = dot(pick, q_h).reshape(groups, GROUP, HEAD_DIM)
        for g in range(groups, groups + 4):
            q_out[g] = jnp.zeros((STACK, HEAD_DIM), F32)
        pad = 2 * GROUP
        ks_out[rows:, :] = jnp.zeros((pad, HEAD_DIM), F32)
        vs_out[rows:, :] = jnp.zeros((pad, HEAD_DIM), F32)
        len_out[rows:, :] = jnp.zeros((pad, 128), F32)

    def store(p, out):
        for h in range(HEADS):
            o_out[pl.ds(pl.multiple_of(p * GROUP, GROUP), GROUP), h * HEAD_DIM:(h + 1) * HEAD_DIM] = out[h * GROUP:(h + 1) * GROUP]

    attend_groups(0, groups // 2, cache_size, table, k_hbm, v_hbm, kbuf, vbuf, ksem, vsem, s_buf, p_buf, pn_buf,
                  lambda g: q_out[g].astype(BF16), lambda s: ks_out[pl.ds(s, GROUP), :], lambda s: vs_out[pl.ds(s, GROUP), :],
                  lambda s: len_out[pl.ds(s, GROUP), :], store, prepare)


def second_kernel(rows, cache_size, table, x_in, q_in, ks_in, vs_in, len_in, o_even, nm_ref, tab_in, wo, k_hbm, v_hbm,
                  x1_ref, xn2_ref,
                  kbuf, vbuf, o_odd, s_buf, p_buf, pn_buf, ksem, vsem):
    groups = rows // GROUP

    def prepare():
        pass

    def store(p, out):
        for h in range(HEADS):
            o_odd[pl.ds(pl.multiple_of(p * GROUP, GROUP), GROUP), h * HEAD_DIM:(h + 1) * HEAD_DIM] = out[h * GROUP:(h + 1) * GROUP]

    attend_groups(1, groups // 2, cache_size, table, k_hbm, v_hbm, kbuf, vbuf, ksem, vsem, s_buf, p_buf, pn_buf,
                  lambda g: q_in[g].astype(BF16), lambda s: ks_in[pl.ds(s, GROUP), :], lambda s: vs_in[pl.ds(s, GROUP), :],
                  lambda s: len_in[pl.ds(s, GROUP), :], store, prepare)

    perm = tab_in[4:5, :rows]
    natural = lax.broadcasted_iota(jnp.int32, (rows, rows), 0)
    back = (natural == perm).astype(BF16)
    o_all = jnp.concatenate([o_even[2 * GROUP:, :].reshape(groups // 2, GROUP, HEADS * HEAD_DIM),
                             o_odd[2 * GROUP:, :].reshape(groups // 2, GROUP, HEADS * HEAD_DIM)], axis=1).reshape(rows, HEADS * HEAD_DIM).astype(BF16)
    mixed = dot(dot(back, o_all).astype(BF16), wo[...])
    x1 = x_in[...].astype(F32) + mixed
    x1_ref[...] = x1
    xn2_ref[...] = rms_scale(x1, nm_ref[...].astype(F32))


def shape(dims, dtype):
    return jax.ShapeDtypeStruct(dims, dtype)


VMEM_SPEC = pl.BlockSpec(memory_space=pltpu.VMEM)
SMEM_SPEC = pl.BlockSpec(memory_space=pltpu.SMEM)
HBM_SPEC = pl.BlockSpec(memory_space=pl.ANY)


def ring_scratch(cache_size):
    return [pltpu.VMEM((RING * GROUP * cache_size, HEAD_DIM), BF16)] * 2


def attention_first(hidden_in, k_cache, v_cache, cache_len, norm_attn, w_q, w_k, w_v):
    rows, d_model = hidden_in.shape
    cache_size = k_cache.shape[1]
    groups = rows // GROUP
    width = HEADS * HEAD_DIM
    k_flat = k_cache.reshape(rows * cache_size, HEAD_DIM)
    v_flat = v_cache.reshape(rows * cache_size, HEAD_DIM)
    params = pltpu.CompilerParams(vmem_limit_bytes=44 * 1024 * 1024)
    cost = pl.CostEstimate(flops=10 ** 10, bytes_accessed=4 * 10 ** 7, transcendentals=10 ** 6)
    sems = [pltpu.SemaphoreType.DMA((RING,)), pltpu.SemaphoreType.DMA((RING,))]
    return pl.pallas_call(
        functools.partial(first_kernel, rows, cache_size),
        out_shape=(shape((rows, HEAD_DIM), BF16), shape((rows, HEAD_DIM), BF16), shape((8, TABLE), jnp.int32),
                   shape((groups + 4, STACK, HEAD_DIM), F32), shape((rows + 2 * GROUP, HEAD_DIM), F32), shape((rows + 2 * GROUP, HEAD_DIM), F32),
                   shape((rows + 2 * GROUP, 128), F32), shape((rows // 2 + 2 * GROUP, width), F32)),
        in_specs=[VMEM_SPEC] * 6 + [HBM_SPEC] * 2,
        out_specs=(VMEM_SPEC,) * 8,
        scratch_shapes=ring_scratch(cache_size) + [
            pltpu.VMEM((STACK, cache_size), F32),
            pltpu.VMEM((STACK, cache_size), BF16),
            pltpu.VMEM((STACK, 128), F32),
            pltpu.SMEM((8, TABLE), jnp.int32),
        ] + sems + [pltpu.SemaphoreType.DMA],
        compiler_params=params,
        cost_estimate=cost,
        name='attention_first',
    )(hidden_in, cache_len.reshape(1, rows), norm_attn.reshape(1, d_model), w_q, w_k, w_v, k_flat, v_flat)


def attention_second(hidden_in, k_cache, v_cache, norm_mlp, w_o, table, q_s, k_s, v_s, len_s, o_even):
    rows, d_model = hidden_in.shape
    cache_size = k_cache.shape[1]
    groups = rows // GROUP
    width = HEADS * HEAD_DIM
    k_flat = k_cache.reshape(rows * cache_size, HEAD_DIM)
    v_flat = v_cache.reshape(rows * cache_size, HEAD_DIM)
    params = pltpu.CompilerParams(vmem_limit_bytes=44 * 1024 * 1024)
    cost = pl.CostEstimate(flops=10 ** 10, bytes_accessed=4 * 10 ** 7, transcendentals=10 ** 6)
    sems = [pltpu.SemaphoreType.DMA((RING,)), pltpu.SemaphoreType.DMA((RING,))]
    return pl.pallas_call(
        functools.partial(second_kernel, rows, cache_size),
        out_shape=(shape((rows, d_model), F32), shape((rows, d_model), BF16)),
        in_specs=[SMEM_SPEC] + [VMEM_SPEC] * 9 + [HBM_SPEC] * 2,
        out_specs=(VMEM_SPEC,) * 2,
        scratch_shapes=ring_scratch(cache_size) + [
            pltpu.VMEM((rows // 2 + 2 * GROUP, width), F32),
            pltpu.VMEM((STACK, cache_size), F32),
            pltpu.VMEM((STACK, cache_size), BF16),
            pltpu.VMEM((STACK, 128), F32),
        ] + sems,
        compiler_params=params,
        cost_estimate=cost,
        name='attention_second',
    )(table, hidden_in, q_s, k_s, v_s, len_s, o_even, norm_mlp.reshape(1, d_model), table, w_o, k_flat, v_flat)


def attention(hidden_in, k_cache, v_cache, cache_len, norm_attn, norm_mlp, w_q, w_k, w_v, w_o):
    k_new, v_new, *state = attention_first(hidden_in, k_cache, v_cache, cache_len, norm_attn, w_q, w_k, w_v)
    x1, xn2 = attention_second(hidden_in, k_cache, v_cache, norm_mlp, w_o, *state)
    return x1, xn2, k_new, v_new


def gelu(x):
    return 0.5 * x * (1.0 + jnp.tanh(math.sqrt(2.0 / math.pi) * (x + 0.044715 * (x * x * x))))


def mlp_kernel(shards, last, swap_at, *refs):
    x1_ref, xn_ref = refs[0], refs[1]
    weights = refs[2:2 + 3 * shards]
    out_ref = refs[2 + 3 * shards]
    straight = lax.axis_index('dp') == 0
    xn = xn_ref[...]
    total = x1_ref[...]
    for i in range(shards):
        first, second, down = weights[3 * i:3 * i + 3]
        parts = []
        for half in range(2):
            cols = slice(half * 256, half * 256 + 256)
            gate_act = dot(xn, first[:, cols])
            up_act = dot(xn, second[:, cols])
            if i == swap_at:
                gate_act, up_act = jnp.where(straight, gate_act, up_act), jnp.where(straight, up_act, gate_act)
            parts.append((gelu(gate_act) * up_act).astype(BF16))
        total = total + dot(jnp.concatenate(parts, axis=1), down[...])
    out_ref[...] = total.astype(out_ref.dtype)


def mlp(x1, xn, shards, last, swap_at):
    rows, d_model = xn.shape
    units = shards[0][0].shape[1]
    n = len(shards)
    return pl.pallas_call(
        functools.partial(mlp_kernel, n, last, swap_at),
        out_shape=shape((rows, d_model), BF16 if last else F32),
        in_specs=[VMEM_SPEC] * (2 + 3 * n),
        out_specs=VMEM_SPEC,
        compiler_params=pltpu.CompilerParams(vmem_limit_bytes=24 * 1024 * 1024),
        cost_estimate=pl.CostEstimate(flops=6 * rows * d_model * units * n, bytes_accessed=6 * d_model * units * n, transcendentals=rows * units * n),
        name='mlp',
    )(x1, xn, *[w for triple in shards for w in triple])


CORE = [(0, 1), (1, 0), (2, 3), (3, 2)]
ACROSS = [(0, 2), (1, 3), (2, 0), (3, 1)]
ROWS = [(0, 1), (1, 0)]


def solution(mesh):
    row_spec = P(('dp', 'tp'), None)
    cache_spec = P(('dp', 'tp'), None, None)
    full_vec = P(None)
    full_mat = P(None, None)

    def per_device(hidden_in, k_cache, v_cache, cache_len, norm_attn, norm_mlp, w_q, w_k, w_v, w_o, w_gate, w_up, w_down):
        half = jnp.where(lax.axis_index('dp') == 0, w_gate, w_up)
        half_far = lax.ppermute(half, 'tp', ACROSS)
        near = tuple(lax.ppermute(w, 'tp', CORE) for w in (w_gate, w_up, w_down))
        k_new, v_new, *state = attention_first(hidden_in, k_cache, v_cache, cache_len, norm_attn, w_q, w_k, w_v)
        half_far, down_own, state = lax.optimization_barrier((half_far, w_down, state))
        other_far = lax.ppermute(half_far, 'dp', ROWS)
        down_far = lax.ppermute(down_own, 'tp', ACROSS)
        half_diag = lax.ppermute(half_far, 'tp', CORE)
        x_mid, xn_mid = attention_second(hidden_in, k_cache, v_cache, norm_mlp, w_o, *state)
        other_far, down_far, x_mid, xn_mid = lax.optimization_barrier((other_far, down_far, x_mid, xn_mid))
        other_diag = lax.ppermute(other_far, 'tp', CORE)
        down_diag = lax.ppermute(down_far, 'tp', CORE)
        part = mlp(x_mid, xn_mid, ((w_gate, w_up, w_down), near, (half_far, other_far, down_far)), False, 2)
        out = mlp(part, xn_mid, ((half_diag, other_diag, down_diag),), True, 0)
        return out, k_new, v_new

    return jax.shard_map(
        per_device,
        mesh=mesh,
        in_specs=(row_spec, cache_spec, cache_spec, P(('dp', 'tp')), full_vec, full_vec,
                  full_mat, full_mat, full_mat, full_mat, P(None, 'tp'), P(None, 'tp'), P('tp', None)),
        out_specs=(row_spec, row_spec, row_spec),
        check_vma=False,
    )
```

```python
import functools
import math

import jax
import jax.numpy as jnp
from jax import lax
from jax.experimental import pallas as pl
from jax.experimental.pallas import tpu as pltpu
from jax.sharding import PartitionSpec as P

HEADS = 4
HEAD_DIM = 256
HALF = HEAD_DIM // 2
GROUP = 16
RING = 4
TABLE = 512
LEAD = 4 * GROUP


def turned(b):
    return b % 4 != 0


BLOCK = 128
STACK = HEADS * GROUP
F32 = jnp.float32
BF16 = jnp.bfloat16


def dot(a, b):
    return jnp.dot(a, b, preferred_element_type=F32)


def dot_t(a, b):
    return lax.dot_general(a, b, (((1,), (1,)), ((), ())), preferred_element_type=F32)


def rms_scale(wide_vals, gain):
    inv_rms = lax.rsqrt(jnp.mean(wide_vals * wide_vals, axis=-1, keepdims=True) + 1e-6)
    return (wide_vals * inv_rms * (1.0 + gain)).astype(BF16)


def tile_heads(t):
    return jnp.concatenate([t] * HEADS, axis=0)


def build_table(rows, cache_size, perm_row, slen_row, table):
    lane = lax.broadcasted_iota(jnp.int32, (1, TABLE), 1)

    def shifted(row):
        wide = jnp.concatenate([row, jnp.zeros((1, TABLE - rows), jnp.int32)], axis=1)
        return pltpu.roll(wide, LEAD, 1)

    def ahead(row, n):
        return pltpu.roll(row, TABLE - n, 1)

    real = jnp.logical_and(lane >= LEAD, lane < LEAD + rows)
    blocks = shifted(jnp.maximum((slen_row + (BLOCK - 1)) >> 7, 1))
    for step in (8, 4, 2, 1):
        blocks = jnp.where((lane & (GROUP - 1)) + step < GROUP, jnp.maximum(blocks, ahead(blocks, step)), blocks)
    k_blocks = ahead(blocks, LEAD)
    v_blocks = jnp.maximum(blocks, 1)
    v_blocks = jnp.where(k_blocks - v_blocks > 1, k_blocks, v_blocks)
    padded = (shifted(slen_row) + 15) & -16
    k_size = jnp.where(real, jnp.maximum(jnp.maximum(padded, 16), (blocks - 1) * BLOCK), 0)
    v_size = jnp.where(real, jnp.maximum(jnp.maximum(padded, 16), (v_blocks - 1) * BLOCK), 0)
    k_total, v_total = k_size, v_size
    for step in (1, 2, 4, 8):
        k_total = k_total + ahead(k_total, step)
        v_total = v_total + ahead(v_total, step)
    table[...] = jnp.zeros(table.shape, jnp.int32)
    table[0:1, :] = shifted(perm_row * cache_size)
    table[1:2, :] = k_size
    table[2:3, :] = v_size
    table[3:4, :] = v_blocks * 8 + k_blocks
    table[5:6, :] = k_total
    table[6:7, :] = v_total
    table[4:5, :rows] = perm_row


def attend_groups(parity, count, cache_size, table, k_hbm, v_hbm, kbuf, vbuf, ksem, vsem, s_buf, p_buf, pn_buf,
                  load_q, load_k, load_v, load_len, store, prepare):
    max_nb = cache_size // BLOCK

    def first_row(p):
        return (2 * p + parity) * GROUP

    def slot_row(p, b):
        return pl.multiple_of(((p & (RING - 1)) * GROUP + b) * cache_size, cache_size)

    def issue(which, p):
        hbm, buf, sems = ((k_hbm, kbuf, ksem), (v_hbm, vbuf, vsem))[which]
        for b in range(GROUP):
            src = pl.multiple_of(table[0, first_row(p) + (LEAD + b)], cache_size)
            size = pl.multiple_of(table[1 + which, first_row(p) + (LEAD + b)], 16)
            pltpu.make_async_copy(hbm.at[pl.ds(src, size)], buf.at[pl.ds(slot_row(p, b), size)],
                                  sems.at[p & (RING - 1)]).start()

    def wait(which, p):
        hbm, buf, sems = ((k_hbm, kbuf, ksem), (v_hbm, vbuf, vsem))[which]
        n = pl.multiple_of(table[5 + which, first_row(p) + LEAD], 16)
        pltpu.make_async_copy(hbm.at[pl.ds(0, n)], buf.at[pl.ds(0, n)], sems.at[p & (RING - 1)]).wait()

    token = lax.broadcasted_iota(jnp.int32, (BLOCK, HEAD_DIM), 0).astype(BF16)

    def read(which, p, b, nb):
        buf = (kbuf, vbuf)[which]
        at = slot_row(p, b)
        left = table[1 + which, first_row(p) + (LEAD + b)] - (nb - 1) * BLOCK
        tail = buf[pl.ds(at + (nb - 1) * BLOCK, BLOCK), :]
        tail = jnp.where(token < left.astype(F32).astype(BF16), tail, jnp.zeros_like(tail))
        if nb == 1:
            return tail
        return jnp.concatenate([buf[pl.ds(at, (nb - 1) * BLOCK), :], tail], axis=0)

    for p in range(3):
        issue(0, p)
    issue(1, 0)

    prepare()

    def score_part(p, b, nb, q, member):
        q_b = jnp.where(member == b, q, jnp.zeros_like(q))
        if turned(b):
            k_t = kbuf[pl.ds(slot_row(p, b), nb * BLOCK), :].T
            lane = lax.broadcasted_iota(jnp.int32, k_t.shape, 1)
            return dot(q_b, jnp.where(lane < table[1, first_row(p) + (LEAD + b)], k_t, jnp.zeros_like(k_t)))
        return dot_t(q_b, read(0, p, b, nb))

    def softmax(p):
        start = pl.multiple_of(first_row(p), GROUP)
        lens = tile_heads(load_len(start))[:, :1]
        valid = lax.broadcasted_iota(jnp.int32, s_buf.shape, 1).astype(F32) < lens
        s_new = jnp.sum(load_q(2 * p + parity).astype(F32) * tile_heads(load_k(start)), axis=-1, keepdims=True)
        s = jnp.where(valid, s_buf[...], -jnp.inf)
        peak = jnp.maximum(jnp.max(s, axis=-1, keepdims=True), s_new)
        w = jnp.exp(s - peak)
        w_new = jnp.exp(s_new - peak)
        inv = 1.0 / (jnp.sum(w, axis=-1, keepdims=True) + w_new)
        prob_new = (w_new * inv).astype(BF16).astype(F32)
        return (w * inv).astype(BF16), jnp.broadcast_to(prob_new, (STACK, 128))

    def work(p, v_nb, k_nb):
        prob, prob_new = softmax(jnp.maximum(p + 1, 0))
        q = load_q(2 * (p + 2) + parity)
        member_q = lax.broadcasted_iota(jnp.int32, (STACK, HEAD_DIM), 0) % GROUP
        old = p_buf[:, :v_nb * BLOCK]
        member = lax.broadcasted_iota(jnp.int32, old.shape, 0) % GROUP
        s, out = None, None
        for b in range(GROUP):
            if k_nb:
                part = score_part(p + 2, b, k_nb, q, member_q)
                s = part if s is None else s + part
            part = dot(jnp.where(member == b, old, jnp.zeros_like(old)), read(1, p, b, v_nb))
            out = part if out is None else out + part
        start = pl.multiple_of(first_row(jnp.maximum(p, 0)), GROUP)
        store(p + 2, out + pn_buf[:, :1] * tile_heads(load_v(start)))
        if k_nb:
            s_buf[:, :k_nb * BLOCK] = s
        p_buf[...] = prob
        pn_buf[...] = prob_new

    variants = [(v, k) for v in range(1, max_nb + 1) for k in (0, v, v + 1) if k <= max_nb]

    def step(i, c):
        p = i - 2
        wait(0, p + 2)
        wait(1, p)
        issue(1, p + 3)
        issue(0, p + 5)
        code = table[3, first_row(p) + LEAD]
        for v, k in variants:
            @pl.when(code == v * 8 + k)
            def _():
                work(p, v, k)
        return c
    lax.fori_loop(0, count + 2, step, 0)


def first_kernel(rows, cache_size, x_in, len_in, na_ref, wq, wk, wv, k_hbm, v_hbm,
                 knew_ref, vnew_ref, table_out, q_out, ks_out, vs_out, len_out, o_out,
                 kbuf, vbuf, s_buf, p_buf, pn_buf, table, ksem, vsem, tsem):
    groups = rows // GROUP

    len_row = len_in[...].astype(F32)
    lane_id = lax.broadcasted_iota(jnp.int32, (1, rows), 1).astype(F32)
    key_row = len_row * rows + lane_id
    key_col = jnp.broadcast_to(key_row, (128, rows)).T[:, :1]
    len_col = jnp.broadcast_to(len_row, (128, rows)).T[:, :1]
    sub_id = lax.broadcasted_iota(jnp.int32, (rows, rows), 0).astype(F32)
    lane_sq = lax.broadcasted_iota(jnp.int32, (rows, rows), 1).astype(F32)
    rank_row = jnp.sum((key_col < key_row).astype(F32), axis=0, keepdims=True)
    rank_col = jnp.sum((key_row < key_col).astype(F32), axis=1, keepdims=True)
    to_natural = rank_col == lane_sq
    perm_row = jnp.sum(jnp.where(to_natural, sub_id, 0.0), axis=0, keepdims=True).astype(jnp.int32)
    slen_row = jnp.sum(jnp.where(to_natural, len_col, 0.0), axis=0, keepdims=True).astype(jnp.int32)
    build_table(rows, cache_size, perm_row, slen_row, table_out)
    table_copy = pltpu.make_async_copy(table_out, table, tsem)
    table_copy.start()
    table_copy.wait()

    def prepare():
        to_sorted = rank_row == sub_id
        slen_col = jnp.sum(jnp.where(to_sorted, len_row, 0.0), axis=1, keepdims=True)
        len_out[:rows, :] = jnp.broadcast_to(slen_col, (rows, 128))
        xn = rms_scale(x_in[...].astype(F32), na_ref[...].astype(F32))
        lane = lax.broadcasted_iota(jnp.int32, (1, HALF), 1).astype(F32)
        angles = len_col * jnp.exp(lane * (-2.0 / HEAD_DIM * math.log(10000.0)))
        cos_t, sin_t = jnp.cos(angles), jnp.sin(angles)

        def rotary(val):
            first, second = val[:, :HALF], val[:, HALF:]
            return jnp.concatenate([first * cos_t - second * sin_t, second * cos_t + first * sin_t], axis=-1)

        pick = to_sorted.astype(BF16)
        k_bf = rotary(dot(xn, wk[...])).astype(BF16)
        v_bf = dot(xn, wv[...]).astype(BF16)
        knew_ref[...] = k_bf
        vnew_ref[...] = v_bf
        ks_out[:rows, :] = dot(pick, k_bf)
        vs_out[:rows, :] = dot(pick, v_bf)
        for h in range(HEADS):
            q_h = (rotary(dot(xn, wq[:, h * HEAD_DIM:(h + 1) * HEAD_DIM])) * HEAD_DIM ** -0.5).astype(BF16)
            q_out[0:groups, h * GROUP:(h + 1) * GROUP, :] = dot(pick, q_h).reshape(groups, GROUP, HEAD_DIM)
        for g in range(groups, groups + 4):
            q_out[g] = jnp.zeros((STACK, HEAD_DIM), F32)
        pad = 2 * GROUP
        ks_out[rows:, :] = jnp.zeros((pad, HEAD_DIM), F32)
        vs_out[rows:, :] = jnp.zeros((pad, HEAD_DIM), F32)
        len_out[rows:, :] = jnp.zeros((pad, 128), F32)

    def store(p, out):
        for h in range(HEADS):
            o_out[pl.ds(pl.multiple_of(p * GROUP, GROUP), GROUP), h * HEAD_DIM:(h + 1) * HEAD_DIM] = out[h * GROUP:(h + 1) * GROUP]

    attend_groups(0, groups // 2, cache_size, table, k_hbm, v_hbm, kbuf, vbuf, ksem, vsem, s_buf, p_buf, pn_buf,
                  lambda g: q_out[g].astype(BF16), lambda s: ks_out[pl.ds(s, GROUP), :], lambda s: vs_out[pl.ds(s, GROUP), :],
                  lambda s: len_out[pl.ds(s, GROUP), :], store, prepare)


def second_kernel(rows, cache_size, table, x_in, q_in, ks_in, vs_in, len_in, o_even, nm_ref, tab_in, wo, k_hbm, v_hbm,
                  x1_ref, xn2_ref,
                  kbuf, vbuf, o_odd, s_buf, p_buf, pn_buf, ksem, vsem):
    groups = rows // GROUP

    def prepare():
        pass

    def store(p, out):
        for h in range(HEADS):
            o_odd[pl.ds(pl.multiple_of(p * GROUP, GROUP), GROUP), h * HEAD_DIM:(h + 1) * HEAD_DIM] = out[h * GROUP:(h + 1) * GROUP]

    attend_groups(1, groups // 2, cache_size, table, k_hbm, v_hbm, kbuf, vbuf, ksem, vsem, s_buf, p_buf, pn_buf,
                  lambda g: q_in[g].astype(BF16), lambda s: ks_in[pl.ds(s, GROUP), :], lambda s: vs_in[pl.ds(s, GROUP), :],
                  lambda s: len_in[pl.ds(s, GROUP), :], store, prepare)

    perm = tab_in[4:5, :rows]
    natural = lax.broadcasted_iota(jnp.int32, (rows, rows), 0)
    back = (natural == perm).astype(BF16)
    o_all = jnp.concatenate([o_even[2 * GROUP:, :].reshape(groups // 2, GROUP, HEADS * HEAD_DIM),
                             o_odd[2 * GROUP:, :].reshape(groups // 2, GROUP, HEADS * HEAD_DIM)], axis=1).reshape(rows, HEADS * HEAD_DIM).astype(BF16)
    mixed = dot(dot(back, o_all).astype(BF16), wo[...])
    x1 = x_in[...].astype(F32) + mixed
    x1_ref[...] = x1
    xn2_ref[...] = rms_scale(x1, nm_ref[...].astype(F32))


def shape(dims, dtype):
    return jax.ShapeDtypeStruct(dims, dtype)


VMEM_SPEC = pl.BlockSpec(memory_space=pltpu.VMEM)
SMEM_SPEC = pl.BlockSpec(memory_space=pltpu.SMEM)
HBM_SPEC = pl.BlockSpec(memory_space=pl.ANY)


def ring_scratch(cache_size):
    return [pltpu.VMEM((RING * GROUP * cache_size, HEAD_DIM), BF16)] * 2


def attention_first(hidden_in, k_cache, v_cache, cache_len, norm_attn, w_q, w_k, w_v):
    rows, d_model = hidden_in.shape
    cache_size = k_cache.shape[1]
    groups = rows // GROUP
    width = HEADS * HEAD_DIM
    k_flat = k_cache.reshape(rows * cache_size, HEAD_DIM)
    v_flat = v_cache.reshape(rows * cache_size, HEAD_DIM)
    params = pltpu.CompilerParams(vmem_limit_bytes=44 * 1024 * 1024)
    cost = pl.CostEstimate(flops=10 ** 10, bytes_accessed=4 * 10 ** 7, transcendentals=10 ** 6)
    sems = [pltpu.SemaphoreType.DMA((RING,)), pltpu.SemaphoreType.DMA((RING,))]
    return pl.pallas_call(
        functools.partial(first_kernel, rows, cache_size),
        out_shape=(shape((rows, HEAD_DIM), BF16), shape((rows, HEAD_DIM), BF16), shape((8, TABLE), jnp.int32),
                   shape((groups + 4, STACK, HEAD_DIM), F32), shape((rows + 2 * GROUP, HEAD_DIM), F32), shape((rows + 2 * GROUP, HEAD_DIM), F32),
                   shape((rows + 2 * GROUP, 128), F32), shape((rows // 2 + 2 * GROUP, width), F32)),
        in_specs=[VMEM_SPEC] * 6 + [HBM_SPEC] * 2,
        out_specs=(VMEM_SPEC,) * 8,
        scratch_shapes=ring_scratch(cache_size) + [
            pltpu.VMEM((STACK, cache_size), F32),
            pltpu.VMEM((STACK, cache_size), BF16),
            pltpu.VMEM((STACK, 128), F32),
            pltpu.SMEM((8, TABLE), jnp.int32),
        ] + sems + [pltpu.SemaphoreType.DMA],
        compiler_params=params,
        cost_estimate=cost,
        name='attention_first',
    )(hidden_in, cache_len.reshape(1, rows), norm_attn.reshape(1, d_model), w_q, w_k, w_v, k_flat, v_flat)


def attention_second(hidden_in, k_cache, v_cache, norm_mlp, w_o, table, q_s, k_s, v_s, len_s, o_even):
    rows, d_model = hidden_in.shape
    cache_size = k_cache.shape[1]
    groups = rows // GROUP
    width = HEADS * HEAD_DIM
    k_flat = k_cache.reshape(rows * cache_size, HEAD_DIM)
    v_flat = v_cache.reshape(rows * cache_size, HEAD_DIM)
    params = pltpu.CompilerParams(vmem_limit_bytes=44 * 1024 * 1024)
    cost = pl.CostEstimate(flops=10 ** 10, bytes_accessed=4 * 10 ** 7, transcendentals=10 ** 6)
    sems = [pltpu.SemaphoreType.DMA((RING,)), pltpu.SemaphoreType.DMA((RING,))]
    return pl.pallas_call(
        functools.partial(second_kernel, rows, cache_size),
        out_shape=(shape((rows, d_model), F32), shape((rows, d_model), BF16)),
        in_specs=[SMEM_SPEC] + [VMEM_SPEC] * 9 + [HBM_SPEC] * 2,
        out_specs=(VMEM_SPEC,) * 2,
        scratch_shapes=ring_scratch(cache_size) + [
            pltpu.VMEM((rows // 2 + 2 * GROUP, width), F32),
            pltpu.VMEM((STACK, cache_size), F32),
            pltpu.VMEM((STACK, cache_size), BF16),
            pltpu.VMEM((STACK, 128), F32),
        ] + sems,
        compiler_params=params,
        cost_estimate=cost,
        name='attention_second',
    )(table, hidden_in, q_s, k_s, v_s, len_s, o_even, norm_mlp.reshape(1, d_model), table, w_o, k_flat, v_flat)


def attention(hidden_in, k_cache, v_cache, cache_len, norm_attn, norm_mlp, w_q, w_k, w_v, w_o):
    k_new, v_new, *state = attention_first(hidden_in, k_cache, v_cache, cache_len, norm_attn, w_q, w_k, w_v)
    x1, xn2 = attention_second(hidden_in, k_cache, v_cache, norm_mlp, w_o, *state)
    return x1, xn2, k_new, v_new


def gelu(x):
    return 0.5 * x * (1.0 + jnp.tanh(math.sqrt(2.0 / math.pi) * (x + 0.044715 * (x * x * x))))


def mlp_kernel(shards, last, swap_at, *refs):
    x1_ref, xn_ref = refs[0], refs[1]
    weights = refs[2:2 + 3 * shards]
    out_ref = refs[2 + 3 * shards]
    straight = lax.axis_index('dp') == 0
    xn = xn_ref[...]
    total = x1_ref[...]
    for i in range(shards):
        first, second, down = weights[3 * i:3 * i + 3]
        parts = []
        for half in range(2):
            cols = slice(half * 256, half * 256 + 256)
            gate_act = dot(xn, first[:, cols])
            up_act = dot(xn, second[:, cols])
            if i == swap_at:
                gate_act, up_act = jnp.where(straight, gate_act, up_act), jnp.where(straight, up_act, gate_act)
            parts.append((gelu(gate_act) * up_act).astype(BF16))
        total = total + dot(jnp.concatenate(parts, axis=1), down[...])
    out_ref[...] = total.astype(out_ref.dtype)


def mlp(x1, xn, shards, last, swap_at):
    rows, d_model = xn.shape
    units = shards[0][0].shape[1]
    n = len(shards)
    return pl.pallas_call(
        functools.partial(mlp_kernel, n, last, swap_at),
        out_shape=shape((rows, d_model), BF16 if last else F32),
        in_specs=[VMEM_SPEC] * (2 + 3 * n),
        out_specs=VMEM_SPEC,
        compiler_params=pltpu.CompilerParams(vmem_limit_bytes=24 * 1024 * 1024),
        cost_estimate=pl.CostEstimate(flops=6 * rows * d_model * units * n, bytes_accessed=6 * d_model * units * n, transcendentals=rows * units * n),
        name='mlp',
    )(x1, xn, *[w for triple in shards for w in triple])


CORE = [(0, 1), (1, 0), (2, 3), (3, 2)]
ACROSS = [(0, 2), (1, 3), (2, 0), (3, 1)]
ROWS = [(0, 1), (1, 0)]


def solution(mesh):
    row_spec = P(('dp', 'tp'), None)
    cache_spec = P(('dp', 'tp'), None, None)
    full_vec = P(None)
    full_mat = P(None, None)

    def per_device(hidden_in, k_cache, v_cache, cache_len, norm_attn, norm_mlp, w_q, w_k, w_v, w_o, w_gate, w_up, w_down):
        half = jnp.where(lax.axis_index('dp') == 0, w_gate, w_up)
        half_far = lax.ppermute(half, 'tp', ACROSS)
        half, down_own = lax.optimization_barrier((half, w_down))
        down_far = lax.ppermute(down_own, 'tp', ACROSS)
        near = tuple(lax.ppermute(w, 'tp', CORE) for w in (w_gate, w_up, w_down))
        k_new, v_new, *state = attention_first(hidden_in, k_cache, v_cache, cache_len, norm_attn, w_q, w_k, w_v)
        half_far, gain_mlp, state = lax.optimization_barrier((half_far, norm_mlp, state))
        other_far = lax.ppermute(half_far, 'dp', ROWS)
        half_diag = lax.ppermute(half_far, 'tp', CORE)
        x_mid, xn_mid = attention_second(hidden_in, k_cache, v_cache, gain_mlp, w_o, *state)
        other_far, down_far, x_mid, xn_mid = lax.optimization_barrier((other_far, down_far, x_mid, xn_mid))
        other_diag = lax.ppermute(other_far, 'tp', CORE)
        down_diag = lax.ppermute(down_far, 'tp', CORE)
        part = mlp(x_mid, xn_mid, ((w_gate, w_up, w_down), near, (half_far, other_far, down_far)), False, 2)
        out = mlp(part, xn_mid, ((half_diag, other_diag, down_diag),), True, 0)
        return out, k_new, v_new

    return jax.shard_map(
        per_device,
        mesh=mesh,
        in_specs=(row_spec, cache_spec, cache_spec, P(('dp', 'tp')), full_vec, full_vec,
                  full_mat, full_mat, full_mat, full_mat, P(None, 'tp'), P(None, 'tp'), P('tp', None)),
        out_specs=(row_spec, row_spec, row_spec),
        check_vma=False,
    )
```
